32 devices in a mesh: section: 2 (over x), ex: 4 (over z), ey: 4 (over y, core).
Axes of the slice: x: 2, y: 2, z: 4, core: 2. Of those that a mesh axis runs over, the one named last changes fastest.
Arguments:
- section_out: bfloat16 [2, 1024, 7168], P('section', ('ex', 'ey')), may hold values from -6 to 6
- expert_ids: int32 [2, 1024, 2], P('section', ('ex', 'ey')), may hold values from 0 to 3, all different within a row; in each aligned block of 64 rows (0 to 63, 64 to 127, ..., all dimensions but the last counted through in order) at most 48 rows name the same one
- gate_weights: float32 [2, 1024, 2], P('section', ('ex', 'ey')), may hold values from 0.1 to 1
- w_gate_up: bfloat16 [2, 4, 7168, 2, 1024], P('section', 'ey', None, None, 'ex'), may hold values from -0.0625 to 0.0625
- w_down: bfloat16 [2, 4, 1024, 7168], P('section', 'ey', 'ex'), may hold values from -0.1875 to 0.1875
Outputs:
- next_state: bfloat16 [2, 1024, 7168], P('section', ('ex', 'ey'))
The draws below stay inside these ranges and needn't reach their ends.
Inputs may be any that keep to these rules, and one draw needn't show every extreme that they name: `expert_ids`: each row names 2 different experts. In the rows of one device (aligned blocks of 64 rows, all leading dimensions in order) no expert is named by more than 48 rows, and some block of every draw names one expert exactly 48 times.
All inputs are finite; a program needn't handle non-finite values.
Results may differ from the reference program's by a relative error of at most 0.008.
Values may be sent and summed in bfloat16 or wider, within the bound.
No kernel may reach another device: no remote copies, remote signals or barrier semaphores. Data moves between devices by JAX's collectives and lax.ppermute only.
A program may use at most 128 MiB of HBM per device.

```python
import math
import jax
import jax.numpy as jnp
import numpy as np
from jax import lax

D = 7168
FF = 1024
TOP = 2
TOK_DEV = 64
SECTIONS = 2
EXPERTS = 4
TOKENS = 1024
CAP = 48
N_EX = 4


def level_of(key, extent, shards, smallest, high):
    loudness, own = 1.0, jax.random.fold_in(key, 6)
    for dim, blocks in shards:
        heights = jnp.exp(jax.random.uniform(jax.random.fold_in(own, dim), (blocks,), jnp.float32, smallest / len(shards), high / len(shards)))
        loudness = loudness * jnp.repeat(heights, extent[dim] // blocks).reshape([-1 if axis == dim else 1 for axis in range(len(extent))])
    return loudness


def shared_out(rng, own, number, rows, number_of, top, reach, slope):
    ranking = jax.random.permutation(rng, number_of)
    crowded, usual = shares(number_of, rows * top, reach, slope, True), shares(number_of, rows * top, reach, slope, False)
    places = jnp.arange(number_of)

    def named(tallies, rotation):
        used = int((tallies > 0).sum())
        fixed = max(1, used // 4)
        shifted = fixed + (places - fixed + rotation * (used - fixed)) % max(1, number_of - fixed)
        return jnp.zeros((number_of,), jnp.int32).at[ranking[jnp.where(places < fixed, places, shifted)]].set(jnp.asarray(tallies, jnp.int32))

    tallies = jnp.where(number % 4 == 0, named(crowded, number // 4), named(usual, number - number // 4 - 1))
    mixed = jax.random.permutation(jax.random.fold_in(own, 3), number_of)
    donor, taker = mixed[0:number_of // 2 * 2:2], mixed[1:number_of // 2 * 2:2]
    room = jnp.minimum(tallies[donor] - 1, reach - tallies[taker]) // 2
    room = jnp.where((donor == ranking[0]) | (taker == ranking[0]) | (tallies[taker] == 0), 0, jnp.maximum(room, 0))
    shifted = jax.random.randint(jax.random.fold_in(own, 4), (number_of // 2,), 0, 1 << 20) % (room + 1)
    tallies = tallies.at[donor].add(-shifted).at[taker].add(shifted)
    items = jnp.searchsorted(jnp.cumsum(tallies), jnp.arange(rows * top), side="right").astype(jnp.int32)
    table = items.reshape(top, rows).T
    table = table[jax.random.permutation(jax.random.fold_in(own, 1), rows)]
    rotation = jax.random.randint(jax.random.fold_in(own, 2), (rows, 1), 0, top)
    return jnp.take_along_axis(table, (jnp.arange(top)[None, :] + rotation) % top, axis=1)


def shares(amount, total, bound, skew, full):
    loads = [(1 << 20) // math.isqrt(standing ** skew) + 1 for standing in range(1, amount + 1)]
    largest = bound if full else min(bound, max(-(-total // amount), total * loads[0] // sum(loads)))
    least = 1 if total - largest >= amount - 1 else 0
    given, spare = [largest] + [least] * (amount - 1), total - largest - least * (amount - 1)
    while spare > 0:
        movable = [i for i in range(1, amount) if given[i] < largest] or [i for i in range(1, amount) if given[i] < bound]
        pool, left = sum([loads[i] for i in movable]), spare
        for i in movable:
            more = min(bound - given[i], max(1, left * loads[i] // pool), spare)
            given[i] = given[i] + more
            spare = spare - more
    return np.array(given)


def centred(key, extent, scale, limit, split=(), held_as=jnp.bfloat16):
    array = scale * jax.random.normal(key, extent, jnp.float32)
    if split:
        array = array * level_of(key, extent, split, -0.22, 0.18)
    return jnp.clip(array, -limit, limit).astype(held_as)


def setup_inputs(seed: int = 0) -> dict:
    key_list = jax.random.split(jax.random.key(seed), 6)
    section_out = centred(key_list[0], (SECTIONS, TOKENS, D), 1.0, 6.0, ((0, 2), (1, 16)))
    expert_ids_keys = jax.random.split(jax.random.fold_in(key_list[1], 1), SECTIONS * TOKENS // TOK_DEV)
    expert_ids_turns = jax.random.permutation(jax.random.fold_in(key_list[1], 3), SECTIONS * TOKENS // TOK_DEV)
    expert_ids = jax.vmap(lambda own, number: shared_out(jax.random.fold_in(key_list[1], 2), own, number, TOK_DEV, EXPERTS, TOP, CAP, 2))(expert_ids_keys, expert_ids_turns).reshape((SECTIONS, TOKENS, TOP))
    gate_weights = jnp.clip(jnp.exp(math.log(1.0) - 2.3025851 * jax.random.uniform(key_list[2], (SECTIONS, TOKENS, TOP), jnp.float32) ** level_of(key_list[2], (SECTIONS, TOKENS, TOP), ((0, 2), (1, 16)), -0.2, 0.2)), 0.1, 1.0)
    w_gate_up = centred(key_list[3], (SECTIONS, EXPERTS, D, 2, FF), D ** -0.5, 0.0625, ((0, 2), (1, 4), (4, 4)))
    w_down = centred(key_list[4], (SECTIONS, EXPERTS, FF, D), FF ** -0.5, 0.1875, ((0, 2), (1, 4), (2, 4)))
    return dict(section_out=section_out, expert_ids=expert_ids, gate_weights=gate_weights, w_gate_up=w_gate_up, w_down=w_down)


def route_section(section_args):
    incoming, chosen_ids, gates, gate_up, down_proj = section_args
    devices = TOKENS // TOK_DEV
    slot_total = devices * CAP
    flat_ids = chosen_ids.reshape(devices, TOK_DEV * TOP)
    one_hot = (flat_ids[:, :, None] == jnp.arange(EXPERTS, dtype=jnp.int32)[None, None, :]).astype(jnp.int32)
    slot_rank = jnp.sum((jnp.cumsum(one_hot, axis=1) - one_hot) * one_hot, axis=2)
    device_ids = jnp.arange(devices, dtype=jnp.int32)[:, None]
    position = (flat_ids * slot_total + device_ids * CAP + slot_rank).reshape(-1).astype(jnp.int32)
    token_of = jnp.arange(TOKENS * TOP, dtype=jnp.int32) // TOP
    source_row = jnp.zeros((EXPERTS * slot_total,), jnp.int32).at[position].set(token_of)
    slice_width = FF // N_EX

    def one_expert(expert_args):
        expert_index, weight_rows, down_rows = expert_args
        chosen_rows = lax.dynamic_slice_in_dim(source_row, expert_index * slot_total, slot_total)
        token_rows = incoming[chosen_rows]
        mixed = jnp.dot(token_rows, weight_rows.reshape(D, 2 * FF), preferred_element_type=jnp.float32)
        hidden = (jax.nn.silu(mixed[:, :FF]) * mixed[:, FF:]).astype(jnp.bfloat16)
        slice_parts = jnp.einsum("rqf,qfd->qrd", hidden.reshape(slot_total, N_EX, slice_width).astype(jnp.float32),
                                 down_rows.reshape(N_EX, slice_width, D).astype(jnp.float32))
        rounded = lax.optimization_barrier(slice_parts.astype(jnp.bfloat16))
        return jnp.sum(rounded.astype(jnp.float32), axis=0).astype(jnp.bfloat16)

    expert_out = lax.map(one_expert, (jnp.arange(EXPERTS, dtype=jnp.int32), gate_up, down_proj))
    picked = expert_out.reshape(EXPERTS * slot_total, D)[position].reshape(TOKENS, TOP, D)
    weighted = jnp.einsum("tkd,tk->td", picked.astype(jnp.float32), gates.astype(jnp.float32))
    return (incoming.astype(jnp.float32) + weighted).astype(jnp.bfloat16)


def reference(section_out, expert_ids, gate_weights, w_gate_up, w_down):
    incoming = jnp.roll(section_out, 1, axis=0)
    return lax.map(route_section, (incoming, expert_ids, gate_weights, w_gate_up, w_down))
```

```python
import jax
import jax.numpy as jnp
from jax import lax
from jax.sharding import PartitionSpec as P

CHUNKS = 2


def on_device(section_out, expert_ids, gate_weights, w_gate_up, w_down):
    tok_rows, width = section_out.shape[1:]
    units = w_down.shape[2]
    sections = lax.axis_size("section")
    n_ex = lax.axis_size("ex")
    experts = lax.axis_size("ey")
    cores = 2 if experts % 2 == 0 else 1
    columns = experts // cores
    ex = lax.axis_index("ex")
    ey = lax.axis_index("ey")
    rows = tok_rows // CHUNKS

    def section_shift(value):
        return lax.ppermute(value, "section", [(s, (s + 1) % sections) for s in range(sections)])

    def ring(value):
        return lax.ppermute(value, "ex", [(q, (q + 1) % n_ex) for q in range(n_ex)])

    def column_shift(value, steps):
        pairs = [
            (c * cores + i, (c + steps) % columns * cores + i)
            for c in range(columns)
            for i in range(cores)
        ]
        return lax.ppermute(value, "ey", pairs)

    def core_swap(value, steps):
        pairs = [
            (c * cores + i, c * cores + (i + steps) % cores)
            for c in range(columns)
            for i in range(cores)
        ]
        return lax.ppermute(value, "ey", pairs)

    incoming = [section_shift(section_out[0, c * rows:(c + 1) * rows]) for c in range(CHUNKS)]

    gate_up = [w_gate_up[0, 0]] + [core_swap(w_gate_up[0, 0], i) for i in range(1, cores)]
    down = [w_down[0, 0]] + [core_swap(w_down[0, 0], i) for i in range(1, cores)]
    down = jnp.concatenate(down, axis=0)

    core = ey % cores
    local = [ey - core + (core - i) % cores for i in range(cores)]
    dense = jnp.sum(
        jnp.where(
            expert_ids[0][:, :, None] == jnp.arange(experts, dtype=jnp.int32)[None, None, :],
            gate_weights[0][:, :, None],
            0.0,
        ),
        axis=1,
    )
    gathered = lax.all_gather(dense, ("ex", "ey"), axis=0, tiled=False)
    gathered = gathered.reshape(n_ex, columns, cores, tok_rows, experts)
    gathered = lax.dynamic_index_in_dim(gathered, core, 2, keepdims=False)
    gathered = jnp.stack(
        [lax.dynamic_index_in_dim(gathered, e, 3, keepdims=False) for e in local], axis=-1
    )

    def unit_gate(back, aside, c):
        column = (ey // cores - aside) % columns
        block = lax.dynamic_index_in_dim(gathered, (ex - back) % n_ex, 0, keepdims=False)
        block = lax.dynamic_index_in_dim(block, column, 0, keepdims=False)
        return block[c * rows:(c + 1) * rows]

    def experts_of(token_rows, gates):
        hidden = []
        for i in range(cores):
            weights = gate_up[i].reshape(width, 2 * units)
            mixed = jnp.dot(token_rows, weights, preferred_element_type=jnp.float32)
            act = jax.nn.silu(mixed[:, :units]) * mixed[:, units:]
            hidden.append((act * gates[:, i:i + 1]).astype(jnp.bfloat16))
        hidden = jnp.concatenate(hidden, axis=1)
        return jnp.dot(hidden, down, preferred_element_type=jnp.float32).astype(jnp.bfloat16)

    results = []
    for c in range(CHUNKS):
        held = {(0, 0): incoming[c]}
        for back in range(n_ex):
            if back:
                held[back, 0] = ring(held[back - 1, 0])
            for aside in range(1, columns):
                held[back, aside] = column_shift(held[back, 0], aside)
        keys = sorted(held, key=lambda key: (-key[1], key[0]))
        out = experts_of(
            jnp.concatenate([held[key] for key in keys], axis=0),
            jnp.concatenate([unit_gate(*key, c) for key in keys], axis=0),
        )
        part = {key: out[n * rows:(n + 1) * rows] for n, key in enumerate(keys)}

        def unit_sum(back):
            total = part[back, 0].astype(jnp.float32)
            for aside in range(1, columns):
                total = total + column_shift(part[back, aside], columns - aside).astype(jnp.float32)
            return total

        total = None
        for back in [*range(1, n_ex), 0]:
            here = unit_sum(back)
            if total is not None:
                here = here + ring(total).astype(jnp.float32)
            total = here.astype(jnp.bfloat16) if back else here
        results.append((incoming[c].astype(jnp.float32) + total).astype(jnp.bfloat16))
    return jnp.concatenate(results, axis=0)[None]


def solution(mesh):
    return jax.shard_map(
        on_device,
        mesh=mesh,
        in_specs=(
            P("section", ("ex", "ey"), None),
            P("section", ("ex", "ey"), None),
            P("section", ("ex", "ey"), None),
            P("section", "ey", None, None, "ex"),
            P("section", "ey", "ex", None),
        ),
        out_specs=P("section", ("ex", "ey"), None),
        check_vma=False,
    )
```

```python
import jax
import jax.numpy as jnp
from jax import lax
from jax.sharding import PartitionSpec as P

CHUNKS = 2


def on_device(section_out, expert_ids, gate_weights, w_gate_up, w_down):
    tok_rows, width = section_out.shape[1:]
    units = w_down.shape[2]
    sections = lax.axis_size("section")
    n_ex = lax.axis_size("ex")
    experts = lax.axis_size("ey")
    cores = 2 if experts % 2 == 0 else 1
    columns = experts // cores
    ey = lax.axis_index("ey")
    rows = tok_rows // CHUNKS

    def section_shift(value):
        return lax.ppermute(value, "section", [(s, (s + 1) % sections) for s in range(sections)])

    def place_shift(value, back, aside):
        pairs = [
            (
                q * experts + c * cores + i,
                (q + back) % n_ex * experts + (c + aside) % columns * cores + i,
            )
            for q in range(n_ex)
            for c in range(columns)
            for i in range(cores)
        ]
        return lax.ppermute(value, ("ex", "ey"), pairs)

    def core_swap(value, steps):
        pairs = [
            (c * cores + i, c * cores + (i + steps) % cores)
            for c in range(columns)
            for i in range(cores)
        ]
        return lax.ppermute(value, "ey", pairs)

    incoming = []
    for c in range(CHUNKS):
        with jax.named_scope(f"shift_{c}"):
            incoming.append(section_shift(section_out[0, c * rows:(c + 1) * rows]))

    gates = jnp.sum(
        jnp.where(
            expert_ids[0].T[None, :, :] == jnp.arange(experts, dtype=jnp.int32)[:, None, None],
            gate_weights[0].T[None, :, :],
            0.0,
        ),
        axis=1,
    )
    core = ey % cores
    local = [ey - core + (core - i) % cores for i in range(cores)]
    keys = [(back, aside) for aside in reversed(range(columns)) for back in range(n_ex)]
    unit_gates = {}
    for key in keys:
        with jax.named_scope("gates"):
            placed = place_shift(gates, *key) if key != (0, 0) else gates
        unit_gates[key] = placed
    stacked = jnp.stack([unit_gates[key] for key in keys], axis=1)
    stacked = stacked.reshape(experts, len(keys), CHUNKS, rows).transpose(0, 2, 1, 3)
    stacked = stacked.reshape(experts, CHUNKS, len(keys) * rows)
    local_gates = [lax.dynamic_index_in_dim(stacked, e, 0, keepdims=False) for e in local]

    own_up = w_gate_up[0, 0].reshape(width, 2 * units)
    with jax.named_scope("swap"):
        gate_up = [own_up] + [core_swap(own_up, i) for i in range(1, cores)]
        down = [w_down[0, 0]] + [core_swap(w_down[0, 0], i) for i in range(1, cores)]

    def experts_of(token_rows, c):
        total = None
        for i in range(cores):
            mixed = jnp.dot(token_rows, gate_up[i], preferred_element_type=jnp.float32)
            act = jax.nn.silu(mixed[:, :units]) * mixed[:, units:]
            hidden = (act * local_gates[i][c][:, None]).astype(jnp.bfloat16)
            part = jnp.dot(hidden, down[i], preferred_element_type=jnp.float32)
            total = part if total is None else total + part
        return total.astype(jnp.bfloat16)

    outs = []
    for c in range(CHUNKS):
        held = {(0, 0): incoming[c]}
        for back in range(n_ex):
            if back:
                with jax.named_scope(f"fz_{c}_{back}"):
                    held[back, 0] = place_shift(held[back - 1, 0], 1, 0)
            source = held[back, 0]
            if c and back == n_ex - 1:
                source, outs[-1] = lax.optimization_barrier((source, outs[-1]))
            for aside in range(1, columns):
                with jax.named_scope(f"fy_{c}_{back}"):
                    held[back, aside] = place_shift(source, 0, aside)
        outs.append(experts_of(jnp.concatenate([held[key] for key in keys], axis=0), c))

    results = []
    for c, out in enumerate(outs):
        part = {key: out[n * rows:(n + 1) * rows] for n, key in enumerate(keys)}
        total = None
        for back in [*range(1, n_ex), 0]:
            here = part[back, 0].astype(jnp.float32)
            for aside in range(1, columns):
                with jax.named_scope(f"ry_{c}_{back}"):
                    here = here + place_shift(part[back, aside], 0, columns - aside).astype(jnp.float32)
            if total is not None:
                with jax.named_scope(f"rz_{c}_{back}"):
                    here = here + place_shift(total, 1, 0).astype(jnp.float32)
            total = here.astype(jnp.bfloat16) if back else here
        results.append((incoming[c].astype(jnp.float32) + total).astype(jnp.bfloat16))
    return jnp.concatenate(results, axis=0)[None]


def solution(mesh):
    return jax.shard_map(
        on_device,
        mesh=mesh,
        in_specs=(
            P("section", ("ex", "ey"), None),
            P("section", ("ex", "ey"), None),
            P("section", ("ex", "ey"), None),
            P("section", "ey", None, None, "ex"),
            P("section", "ey", "ex", None),
        ),
        out_specs=P("section", ("ex", "ey"), None),
        check_vma=False,
    )
```

```python
import jax
import jax.numpy as jnp
from jax import lax
from jax.sharding import PartitionSpec as P


def tie(*values):
    return lax.optimization_barrier(values)


def on_device(section_out, expert_ids, gate_weights, w_gate_up, w_down):
    tok_rows, width = section_out.shape[1:]
    units = w_down.shape[2]
    sections = lax.axis_size("section")
    n_ex = lax.axis_size("ex")
    experts = lax.axis_size("ey")
    cores = 2 if experts % 2 == 0 else 1
    columns = experts // cores
    ey = lax.axis_index("ey")
    rows = tok_rows // 2
    relay = n_ex > 2
    last = n_ex - 1
    asides = range(1, columns)

    def section_shift(value):
        pairs = [(s, (s + 1) % sections) for s in range(sections)]
        return lax.ppermute(value, "section", pairs)

    def place_shift(value, back, aside):
        pairs = [
            (
                q * experts + c * cores + i,
                (q + back) % n_ex * experts + (c + aside) % columns * cores + i,
            )
            for q in range(n_ex)
            for c in range(columns)
            for i in range(cores)
        ]
        return lax.ppermute(value, ("ex", "ey"), pairs)

    def core_swap(value, steps):
        pairs = [
            (c * cores + i, c * cores + (i + steps) % cores)
            for c in range(columns)
            for i in range(cores)
        ]
        return lax.ppermute(value, "ey", pairs)

    incoming = [section_shift(section_out[0, c * rows:(c + 1) * rows]) for c in range(2)]

    gates = jnp.sum(
        jnp.where(
            expert_ids[0].T[None, :, :] == jnp.arange(experts, dtype=jnp.int32)[:, None, None],
            gate_weights[0].T[None, :, :],
            0.0,
        ),
        axis=1,
    )
    core = ey % cores
    local = [ey - core + (core - i) % cores for i in range(cores)]
    keys = [(back, aside) for aside in reversed(range(columns)) for back in range(n_ex)]
    placed = [place_shift(gates, *key) if key != (0, 0) else gates for key in keys]
    stacked = jnp.stack(placed, axis=1).reshape(experts, len(keys), 2, rows)
    stacked = stacked.transpose(0, 2, 1, 3).reshape(experts, 2, len(keys) * rows)
    local_gates = [lax.dynamic_index_in_dim(stacked, e, 0, keepdims=False) for e in local]

    own_up = w_gate_up[0, 0].reshape(width, 2 * units)
    incoming[0], own_up = tie(incoming[0], own_up)
    gate_up = [own_up] + [core_swap(own_up, i) for i in range(1, cores)]
    down = [w_down[0, 0]] + [core_swap(w_down[0, 0], i) for i in range(1, cores)]

    held = [{(0, 0): incoming[c]} for c in range(2)]

    def step_z(c, back):
        held[c][back, 0] = place_shift(held[c][back - 1, 0], 1, 0)

    def step_y(c, back):
        for aside in asides:
            held[c][back, aside] = place_shift(held[c][back, 0], 0, aside)

    def hidden_of(c):
        token_rows = jnp.concatenate([held[c][key] for key in keys], axis=0)
        hidden = []
        for i in range(cores):
            mixed = jnp.dot(token_rows, gate_up[i], preferred_element_type=jnp.float32)
            act = jax.nn.silu(mixed[:, :units]) * mixed[:, units:]
            hidden.append((act * local_gates[i][c][:, None]).astype(jnp.bfloat16))
        return hidden

    def parts_of(hidden):
        total = None
        for i in range(cores):
            part = jnp.dot(hidden[i], down[i], preferred_element_type=jnp.float32)
            total = part if total is None else total + part
        out = total.astype(jnp.bfloat16)
        return {key: out[n * rows:(n + 1) * rows] for n, key in enumerate(keys)}

    for back in range(n_ex):
        if back:
            step_z(0, back)
        step_y(0, back)
    late = [key for key in keys if key[1] or key == (last, 0)]
    held[0].update(zip(late, tie(*[held[0][key] for key in late])))
    hidden = [hidden_of(0), None]
    for back in range(n_ex):
        if back:
            step_z(1, back)
            if back == last:
                held[1][last, 0], *hidden[0] = tie(held[1][last, 0], *hidden[0])
        if relay and back == 1:
            for aside in asides:
                held[1][1, aside] = place_shift(held[1][0, aside], 1, 0)
        else:
            step_y(1, back)
    part = [parts_of(hidden[0]), None]
    late = [key for key in keys if key[1]]
    if late:
        sent = part[0][late[0]]
        sent, *moved = tie(sent, *[held[1][key] for key in late])
        part[0][late[0]] = sent
        held[1].update(zip(late, moved))
    hidden[1] = hidden_of(1)
    if relay:
        for aside in asides:
            moved = place_shift(part[0][1, aside], 1, 0)
            moved, hidden[1][0] = tie(moved, hidden[1][0])
            part[0][2, aside] = part[0][2, aside] + moved
    part[1] = parts_of(hidden[1])

    results = []
    for c in range(2):
        total = None
        for back in [*range(1, n_ex), 0]:
            here = part[c][back, 0].astype(jnp.float32)
            if not (relay and c == 0 and back == 1):
                for aside in asides:
                    here = here + place_shift(
                        part[c][back, aside], 0, columns - aside
                    ).astype(jnp.float32)
            if total is not None:
                here = here + place_shift(total, 1, 0).astype(jnp.float32)
            total = here.astype(jnp.bfloat16) if back else here
        results.append((incoming[c].astype(jnp.float32) + total).astype(jnp.bfloat16))
    return jnp.concatenate(results, axis=0)[None]


def solution(mesh):
    return jax.shard_map(
        on_device,
        mesh=mesh,
        in_specs=(
            P("section", ("ex", "ey"), None),
            P("section", ("ex", "ey"), None),
            P("section", ("ex", "ey"), None),
            P("section", "ey", None, None, "ex"),
            P("section", "ey", "ex", None),
        ),
        out_specs=P("section", ("ex", "ey"), None),
        check_vma=False,
    )
```
